32 devices in a mesh: pair: 4 (over x, core), aux: 8 (over z, y).
Axes of the slice: x: 2, y: 2, z: 4, core: 2. Of those that a mesh axis runs over, the one named last changes fastest.
Arguments:
- left_active: bfloat16 [40, 128, 61440], P('pair', None, 'aux'), may hold values from -0.375 to 0.375
- right_active: bfloat16 [40, 128, 61440], P('pair', None, 'aux'), may hold values from -0.375 to 0.375
- amps_active: bfloat16 [40, 128, 128], P('pair', 'aux'), may hold values from -0.5 to 0.5
- rank_active: int32 [40], P('pair'), may hold values from 80 to 128, as said below
- gap_active: float32 [40], P('pair'), may hold values from 0.5 to 2
- energy_active: float32 [40, 128], P('pair'), may hold values from 0.5 to 4
- intersect_active: bfloat16 [40, 4, 128, 128], P('pair'), may hold values from -0.75 to 0.75
- fock_active: float32 [40, 4], P('pair'), may hold values from -2 to 2
- neighbor_active: int32 [40, 4], P('pair'), may hold values from 0 to 39
- left_env: bfloat16 [16, 48, 61440], P('pair', None, 'aux'), may hold values from -0.375 to 0.375
- right_env: bfloat16 [16, 48, 61440], P('pair', None, 'aux'), may hold values from -0.375 to 0.375
- amps_env: bfloat16 [16, 48, 48], P('pair', 'aux'), may hold values from -0.875 to 0.875
- rank_env: int32 [16], P('pair'), may hold values from 24 to 48, as said below
- gap_env: float32 [16], P('pair'), may hold values from 0.5 to 2
- energy_env: float32 [16, 48], P('pair'), may hold values from 0.5 to 4
- intersect_env: bfloat16 [16, 4, 48, 48], P('pair'), may hold values from -1.25 to 1.25
- fock_env: float32 [16, 4], P('pair'), may hold values from -2 to 2
- neighbor_env: int32 [16, 4], P('pair'), may hold values from 0 to 15
Outputs:
- new_active: float32 [40, 128, 128], P('pair', 'aux')
- new_env: float32 [16, 48, 48], P('pair', 'aux')
The draws below stay inside these ranges and needn't reach their ends.
Inputs may be any that keep to these rules, and one draw needn't show every extreme that they name: `rank_active`: multiples of 8; the first active pair has rank 128. `rank_env`: multiples of 8; the first environment pair has rank 48.
All inputs are finite; a program needn't handle non-finite values.
Results may differ from the reference program's by a relative error of at most 0.0041.
Values may be sent and summed in bfloat16 or wider, within the bound.
A program may use at most 128 MiB of HBM per device.

```python
import math
import jax
import jax.numpy as jnp
from jax import lax

RA = 128
RE = 48
NAUX = 61440
NB = 4
PA = 40
PE = 16


def draw_rank_active(key, part):
    values = 8 * jax.random.randint(key, (PA,), RA * 5 // 64, RA // 8 + 1)
    return values.at[0].set(RA).astype(jnp.int32)


def draw_rank_env(key, part):
    values = 8 * jax.random.randint(key, (PE,), RE // 16, RE // 8 + 1)
    return values.at[0].set(RE).astype(jnp.int32)


def set_ends(array, key, least, high):
    longest = array.shape.index(max(array.shape))
    spots = []
    for shift in (0, 1):
        where = [jax.random.randint(jax.random.fold_in(key, axis), (), 0, length) for axis, length in enumerate(array.shape)]
        where[longest] = (where[longest] + shift) % array.shape[longest]
        spots.append(tuple(where))
    return array.at[spots[0]].set(least).at[spots[1]].set(high)


def block_scale(own_key, extent, shards, least, largest):
    factor_of = 1.0
    for position, blocks in shards:
        steps = jax.random.uniform(jax.random.fold_in(jax.random.fold_in(own_key, 6), position), (blocks,), jnp.float32, least / len(shards), largest / len(shards))
        factor_of = factor_of * jnp.repeat(jnp.exp(steps), extent[position] // blocks).reshape((-1,) + (1,) * (len(extent) - 1 - position))
    return factor_of


def normal_values(own_key, dims, width, most, pieces=(), held_as=jnp.bfloat16):
    factor_of = block_scale(own_key, dims, pieces, -0.22, 0.18) if pieces else 1.0
    entries = jax.random.normal(own_key, dims, jnp.float32) * width * factor_of
    return jnp.minimum(jnp.maximum(entries, -most), most).astype(held_as)


def setup_inputs(seed: int = 0) -> dict:
    key_list = jax.random.split(jax.random.key(seed), 19)
    left_active = normal_values(key_list[0], (PA, RA, NAUX), (NAUX ** -0.25), 0.375, ((0, 4), (2, 8)))
    right_active = normal_values(key_list[1], (PA, RA, NAUX), (NAUX ** -0.25), 0.375, ((0, 4), (2, 8)))
    amps_active = normal_values(key_list[2], (PA, RA, RA), (RA ** -0.5), 0.5, ((0, 4), (1, 8)))
    rank_active = draw_rank_active(jax.random.fold_in(key_list[18], 71), 0)
    gap_active = jnp.clip(jnp.exp(math.log(2.0) - 1.3862944 * jax.random.uniform(key_list[4], (PA,), jnp.float32) ** block_scale(key_list[4], (PA,), ((0, 4),), -0.2, 0.2)), 0.5, 2.0)
    energy_active = jnp.clip(jnp.exp(math.log(4.0) - 2.0794415 * jax.random.uniform(key_list[5], (PA, RA), jnp.float32) ** block_scale(key_list[5], (PA, RA), ((0, 4),), -0.2, 0.2)), 0.5, 4.0)
    intersect_active = normal_values(key_list[6], (PA, NB, RA, RA), (RA // 2) ** -0.5, 0.75, ((0, 4),))
    fock_active = jnp.clip(jax.random.uniform(key_list[7], (PA, NB), jnp.float32, -2.0, 2.0) * block_scale(key_list[7], (PA, NB), ((0, 4),), -0.4, 0.0), -2.0, 2.0)
    neighbor_active = set_ends(jax.random.randint(key_list[8], (PA, NB), 0, PA), jax.random.fold_in(key_list[8], 1), 0, PA - 1).astype(jnp.int32)
    left_env = normal_values(key_list[9], (PE, RE, NAUX), (NAUX ** -0.25), 0.375, ((0, 4), (2, 8)))
    right_env = normal_values(key_list[10], (PE, RE, NAUX), (NAUX ** -0.25), 0.375, ((0, 4), (2, 8)))
    amps_env = normal_values(key_list[11], (PE, RE, RE), (RE ** -0.5), 0.875, ((0, 4), (1, 8)))
    rank_env = draw_rank_env(jax.random.fold_in(key_list[18], 71), 0)
    gap_env = jnp.clip(jnp.exp(math.log(2.0) - 1.3862944 * jax.random.uniform(key_list[13], (PE,), jnp.float32) ** block_scale(key_list[13], (PE,), ((0, 4),), -0.2, 0.2)), 0.5, 2.0)
    energy_env = jnp.clip(jnp.exp(math.log(4.0) - 2.0794415 * jax.random.uniform(key_list[14], (PE, RE), jnp.float32) ** block_scale(key_list[14], (PE, RE), ((0, 4),), -0.2, 0.2)), 0.5, 4.0)
    intersect_env = normal_values(key_list[15], (PE, NB, RE, RE), (RE // 2) ** -0.5, 1.25, ((0, 4),))
    fock_env = jnp.clip(jax.random.uniform(key_list[16], (PE, NB), jnp.float32, -2.0, 2.0) * block_scale(key_list[16], (PE, NB), ((0, 4),), -0.4, 0.0), -2.0, 2.0)
    neighbor_env = set_ends(jax.random.randint(key_list[17], (PE, NB), 0, PE), jax.random.fold_in(key_list[17], 1), 0, PE - 1).astype(jnp.int32)
    return dict(left_active=left_active, right_active=right_active, amps_active=amps_active, rank_active=rank_active, gap_active=gap_active, energy_active=energy_active, intersect_active=intersect_active, fock_active=fock_active, neighbor_active=neighbor_active, left_env=left_env, right_env=right_env, amps_env=amps_env, rank_env=rank_env, gap_env=gap_env, energy_env=energy_env, intersect_env=intersect_env, fock_env=fock_env, neighbor_env=neighbor_env)


HIGHEST = lax.Precision.HIGHEST


def rank_masks(pair_ranks, full_width):
    positions = jnp.arange(full_width, dtype=jnp.int32)
    return (positions[None, :, None] < pair_ranks[:, None, None]) & (positions[None, None, :] < pair_ranks[:, None, None])


def update_level(left_ints, right_ints, amplitudes, pair_ranks, pair_gaps, energy, intersect, fock_weights, neighbor, with_ladder):
    full_width = amplitudes.shape[1]
    inside = rank_masks(pair_ranks, full_width)
    masked = jnp.where(inside, amplitudes, jnp.zeros_like(amplitudes))

    def one_pair(pair_items):
        left_pair, right_pair, amp_pair, over_pair, fock_pair, neigh_pair = pair_items
        summed_terms = jnp.dot(left_pair, right_pair.T, preferred_element_type=jnp.float32)
        if with_ladder:
            cross_left = jnp.dot(amp_pair.T, left_pair, preferred_element_type=jnp.float32).astype(jnp.bfloat16)
            cross_right = jnp.dot(amp_pair, right_pair, preferred_element_type=jnp.float32).astype(jnp.bfloat16)
            summed_terms = summed_terms + jnp.dot(cross_left, right_pair.T, preferred_element_type=jnp.float32)
            summed_terms = summed_terms + jnp.dot(cross_left, cross_right.T, preferred_element_type=jnp.float32)
        near_amps = masked[neigh_pair]
        half_product = jnp.einsum('krs,kst->krt', over_pair, near_amps, preferred_element_type=jnp.float32)
        full_product = jnp.einsum('krt,kut->kru', half_product, over_pair.astype(jnp.float32), precision=HIGHEST)
        return summed_terms + jnp.einsum('k,kru->ru', fock_pair, full_product, precision=HIGHEST)

    residual = lax.map(one_pair, (left_ints, right_ints, masked, intersect, fock_weights, neighbor))
    denominator = energy[:, :, None] + energy[:, None, :] + pair_gaps[:, None, None]
    return jnp.where(inside, masked.astype(jnp.float32) - residual / denominator, jnp.float32(0.0))


def reference(left_active, right_active, amps_active, rank_active, gap_active, energy_active, intersect_active, fock_active, neighbor_active, left_env, right_env, amps_env, rank_env, gap_env, energy_env, intersect_env, fock_env, neighbor_env):
    new_active = update_level(left_active, right_active, amps_active, rank_active, gap_active, energy_active, intersect_active, fock_active, neighbor_active, True)
    new_env = update_level(left_env, right_env, amps_env, rank_env, gap_env, energy_env, intersect_env, fock_env, neighbor_env, False)
    return (new_active, new_env)
```

```python
import functools

import jax
import jax.numpy as jnp
from jax import lax
from jax.experimental import pallas as pl
from jax.experimental.pallas import tpu as pltpu
from jax.sharding import PartitionSpec as P

BF = jnp.bfloat16
F32 = jnp.float32
LANES = 128
AHEAD = 4
WARM = 5
LATE = 2


def dot_nt(x, y):
    return lax.dot_general(x, y, (((1,), (1,)), ((), ())), preferred_element_type=F32)


def split(x):
    hi = x.astype(BF)
    return hi, (x - hi.astype(F32)).astype(BF)


def iota2(shape, dim):
    return lax.broadcasted_iota(jnp.int32, shape, dim)


def half_couple(over, near, fock, place, rows, step):
    width = over[0].shape[1]
    pick = (iota2((step, width), 1) == place * rows + iota2((step, width), 0)) & (
        iota2((step, width), 0) < rows
    )
    pick = jnp.where(pick, F32(1.0), F32(0.0))
    lefts, rights = [], []
    for k in range(len(over)):
        both = dot_nt(jnp.concatenate([pick, near[k]], axis=0).astype(BF), over[k])
        lefts.append(both[:step])
        rights.append(both[step:] * fock[k])
    return jnp.concatenate(lefts, axis=0).astype(BF), jnp.concatenate(rights, axis=0).astype(BF)


def dot_tn(x, y):
    return lax.dot_general(x, y, (((0,), (0,)), ((), ())), preferred_element_type=F32)


def far_first(n):
    return sorted(range(1, n), key=lambda d: -min(d, n - d))


def kernel(
    n_pair, n_aux,
    la, ra, aa, rka_h, gpa_h, ena_h, ina, fka_h, nba_h,
    le, re, ae_h, rke_h, gpe_h, ene_h, ine_h, fke_h, nbe_h,
    oa, oe,
    lbuf, rbuf, lebuf, rebuf, inbuf, aabuf, ae, ena, ene, ine,
    rka, gpa, fka, nba, rke, gpe, fke, nbe,
    mine, own, around, mine_e, around_e,
    terms, out_a, in_a, terms_e, out_e, in_e, den, den_e,
    lefts, rights,
    lr_sem, lre_sem, in_sem, small_sem,
    own_send, own_recv, pair_send, pair_recv, paire_send, paire_recv,
    a_send, a_recv, e_send, e_recv,
):
    pairs, rows, full = mine.shape
    rows_e, pairs_e, full_e = ae.shape
    pad_e = mine_e.shape[1]
    count = nba.shape[0]
    warm = min(WARM, pairs - 1)
    late = pairs - LATE
    me = lax.axis_index("aux")
    my_pair = lax.axis_index("pair")
    order = far_first(n_aux)

    def load_lr(p):
        return (
            pltpu.make_async_copy(la.at[p], lbuf.at[p], lr_sem.at[p, 0]),
            pltpu.make_async_copy(ra.at[p], rbuf.at[p], lr_sem.at[p, 1]),
        )

    def load_e(q):
        return (
            pltpu.make_async_copy(le.at[q], lebuf.at[q], lre_sem.at[q, 0]),
            pltpu.make_async_copy(re.at[q], rebuf.at[q], lre_sem.at[q, 1]),
        )

    def start_load(i):
        if isinstance(i, int):
            if i < pairs:
                for copy in load_lr(i):
                    copy.start()
            elif i < pairs + pairs_e:
                for copy in load_e(i - pairs):
                    copy.start()
        else:
            @pl.when(i < pairs)
            def _():
                for copy in load_lr(i):
                    copy.start()

            @pl.when((i >= pairs) & (i < pairs + pairs_e))
            def _():
                for copy in load_e(i - pairs):
                    copy.start()

    small = [(aa, aabuf), (rka_h, rka), (ae_h, ae), (rke_h, rke)]
    rest = [
        (gpa_h, gpa), (ena_h, ena), (fka_h, fka), (nba_h, nba), (gpe_h, gpe), (ene_h, ene),
        (ine_h, ine), (fke_h, fke), (nbe_h, nbe),
    ]
    copies = [pltpu.make_async_copy(x, y, small_sem.at[i]) for i, (x, y) in enumerate(small + rest)]
    for copy in copies[: len(small)]:
        copy.start()
    barrier = pltpu.get_barrier_semaphore()
    for d in order:
        pl.semaphore_signal(barrier, inc=1, device_id={"aux": lax.rem(me + d, n_aux)}, device_id_type=pl.DeviceIdType.MESH)
    for d in range(1, n_pair):
        pl.semaphore_signal(barrier, inc=1, device_id={"pair": lax.rem(my_pair + d, n_pair)}, device_id_type=pl.DeviceIdType.MESH)
    for i in range(AHEAD):
        start_load(i)
    for copy in copies[len(small) :]:
        copy.start()
    load_in = pltpu.make_async_copy(ina, inbuf, in_sem)
    load_in.start()
    for copy in copies[: len(small)]:
        copy.wait()

    def inside(rank, start, shape):
        return (start + iota2(shape, 0) < rank) & (iota2(shape, 1) < rank)

    for p in range(pairs):
        keep = inside(rka[p], me * rows, (rows, full))
        block = jnp.where(keep, aabuf[p].astype(F32), F32(0.0)).astype(BF)
        mine[p] = block
        own[me, p] = block
        around[my_pair * pairs + p] = block
    mine_e[...] = jnp.zeros(mine_e.shape, F32)
    amps_e = ae[...].astype(F32)
    for p in range(pairs_e):
        keep = inside(rke[p], me * rows_e, (rows_e, full_e))
        mine_e[p, :rows_e, :full_e] = jnp.where(keep, amps_e[:, p, :], F32(0.0))
    for p in range(pairs_e):
        around_e[my_pair * pairs_e + p] = mine_e[p]
    out_e[...] = jnp.zeros(out_e.shape, out_e.dtype)

    def to_own(d, slot):
        return pltpu.make_async_remote_copy(
            src_ref=mine, dst_ref=own.at[slot],
            send_sem=own_send.at[d - 1], recv_sem=own_recv.at[d - 1],
            device_id={"aux": lax.rem(me + d, n_aux)}, device_id_type=pl.DeviceIdType.MESH,
        )

    def to_pair(d, slot):
        return pltpu.make_async_remote_copy(
            src_ref=mine, dst_ref=around.at[pl.ds(slot * pairs, pairs)],
            send_sem=pair_send.at[d - 1], recv_sem=pair_recv.at[d - 1],
            device_id={"pair": lax.rem(my_pair + d, n_pair)}, device_id_type=pl.DeviceIdType.MESH,
        )

    def to_pair_e(d, slot):
        return pltpu.make_async_remote_copy(
            src_ref=mine_e, dst_ref=around_e.at[pl.ds(slot * pairs_e, pairs_e)],
            send_sem=paire_send.at[d - 1], recv_sem=paire_recv.at[d - 1],
            device_id={"pair": lax.rem(my_pair + d, n_pair)}, device_id_type=pl.DeviceIdType.MESH,
        )

    pl.semaphore_wait(barrier, n_aux - 1 + n_pair - 1)
    for d in order:
        to_own(d, me).start()
    for d in range(1, n_pair):
        to_pair(d, my_pair).start()
        to_pair_e(d, my_pair).start()

    def denominators(energy, gap, start, height, wide):
        line = energy + jnp.zeros((height, wide), F32)
        diag = iota2((height, wide), 1) == start + iota2((height, wide), 0)
        mine_rows = jnp.sum(jnp.where(diag, line, F32(0.0)), axis=1, keepdims=True)
        return line + mine_rows + gap

    def a_copy(d, p, group):
        peer = lax.rem(me + d, n_aux)
        return pltpu.make_async_remote_copy(
            src_ref=out_a.at[peer, p], dst_ref=in_a.at[d - 1, p],
            send_sem=a_send.at[d - 1, group], recv_sem=a_recv.at[d - 1, group],
            device_id={"aux": peer}, device_id_type=pl.DeviceIdType.MESH,
        )

    def e_copy(d):
        peer = lax.rem(me + d, n_aux)
        return pltpu.make_async_remote_copy(
            src_ref=out_e.at[peer], dst_ref=in_e.at[d - 1],
            send_sem=e_send.at[d - 1], recv_sem=e_recv.at[d - 1],
            device_id={"aux": peer}, device_id_type=pl.DeviceIdType.MESH,
        )

    def send_pair(p, group):
        for d in order:
            a_copy(d, p, group).start()

    def integrals(p):
        for copy in load_lr(p):
            copy.wait()
        return dot_nt(lbuf[p], rbuf[p])

    def ladder(p):
        terms[p] = integrals(p).reshape(n_aux, rows, full)

    def prepare(p):
        left, right = half_couple(
            [inbuf[p, k] for k in range(count)],
            [around[nba[k, p]].astype(F32) for k in range(count)],
            [fka[k, p] for k in range(count)],
            me, rows, rows,
        )
        lefts[p] = left
        rights[p] = right

    def finish(p):
        base = terms[p].reshape(full, full)
        amps = own[:, p].astype(F32).reshape(full, full).astype(BF)
        half = base + dot_nt(base.astype(BF), amps)
        total = base + dot_tn(
            jnp.concatenate([amps, lefts[p]], axis=0),
            jnp.concatenate([half.astype(BF), rights[p]], axis=0),
        )
        terms[p] = total.reshape(n_aux, rows, full)
        for j in range(n_aux):
            out_a[j, p] = total[j * rows : (j + 1) * rows].astype(BF)

    def warm_step(p, carry):
        start_load(p + AHEAD)
        ladder(p)
        return carry

    lax.fori_loop(0, warm, warm_step, 0)

    for copy in copies[len(small) :]:
        copy.wait()
    load_in.wait()
    for d in range(1, n_pair):
        slot = lax.rem(my_pair + n_pair - d, n_pair)
        to_pair(d, slot).wait_recv()
        to_pair_e(d, slot).wait_recv()

    def prepare_step(p, carry):
        prepare(p)
        return carry

    lax.fori_loop(0, pairs, prepare_step, 0)
    for q in range(pairs_e):
        left, right = half_couple(
            [ine[q, k] for k in range(count)],
            [around_e[nbe[q, k]][:, :full_e] for k in range(count)],
            [fke[q, k] for k in range(count)],
            me, rows_e, pad_e,
        )
        terms_e[q] = dot_tn(left, right)
    for p in range(pairs):
        den[p] = denominators(ena[pl.ds(p, 1), :], gpa[p], me * rows, rows, full)
    for p in range(pairs_e):
        den_e[p] = denominators(ene[pl.ds(p, 1), :], gpe[p], me * rows_e, rows_e, full_e)
    for d in range(1, n_aux):
        to_own(d, lax.rem(me + n_aux - d, n_aux)).wait_recv()

    twos = min(pairs - 1 - warm, max(0, warm - 1))

    def catch_step(i, carry):
        p = warm + i
        start_load(p + AHEAD)

        @pl.when(i > 0)
        def _():
            send_pair(2 * i - 2, 0)
            send_pair(2 * i - 1, 0)

        ladder(p)
        finish(2 * i)
        finish(2 * i + 1)
        return carry

    lax.fori_loop(0, twos, catch_step, 0)
    done = 2 * twos
    sent = max(0, done - 2)
    for p in range(warm + twos, pairs):
        start_load(p + AHEAD)
        for q in range(sent, done):
            send_pair(q, int(q >= late))
        sent = done
        ladder(p)
        if done < p:
            finish(done)
            done += 1
    for i in range(pairs + AHEAD, pairs + pairs_e):
        start_load(i)
    for q in range(sent, done):
        send_pair(q, int(q >= late))
    sent = done
    while done < pairs:
        finish(done)
        done += 1
    for q in range(pairs_e):
        for copy in load_e(q):
            copy.wait()
        total = terms_e[q] + dot_nt(lebuf[q], rebuf[q])
        terms_e[q] = total
        for j in range(n_aux):
            out_e[j, q, :rows_e, :full_e] = total[j * rows_e : (j + 1) * rows_e, :].astype(out_e.dtype)
        if q == 0:
            for p in range(sent, pairs):
                send_pair(p, int(p >= late))

    def combine(p):
        total = terms[p, me]
        for d in range(1, n_aux):
            total = total + in_a[d - 1, p].astype(F32)
        keep = inside(rka[p], me * rows, (rows, full))
        oa[p] = jnp.where(keep, mine[p].astype(F32) - total / den[p], F32(0.0))

    def arrived(group):
        block = in_a.at[:, pl.ds(0, late)] if group == 0 else in_a.at[:, pl.ds(late, pairs - late)]
        return [
            pltpu.make_async_copy(block.at[d - 1], block.at[d - 1], a_recv.at[d - 1, group])
            for d in range(1, n_aux)
        ]

    for d in order:
        e_copy(d).start()
    for copy in arrived(0):
        copy.wait()
    for p in range(late):
        combine(p)
    for copy in arrived(1):
        copy.wait()
    for p in range(late, pairs):
        combine(p)

    for d in range(1, n_aux):
        e_copy(d).wait_recv()
    for p in range(pairs_e):
        total = out_e[me, p].astype(F32)
        for d in range(1, n_aux):
            total = total + in_e[d - 1, p].astype(F32)
        keep = inside(rke[p], me * rows_e, (rows_e, full_e))
        oe[:, p, :] = jnp.where(
            keep, mine_e[p, :rows_e, :full_e] - total[:rows_e, :full_e] / den_e[p], F32(0.0)
        )

    for d in range(1, n_pair):
        to_pair(d, my_pair).wait_send()
        to_pair_e(d, my_pair).wait_send()
    for d in range(1, n_aux):
        to_own(d, me).wait_send()
        e_copy(d).wait_send()
        for group, block in ((0, in_a.at[:, pl.ds(0, late)]), (1, in_a.at[:, pl.ds(late, pairs - late)])):
            pltpu.make_async_copy(block.at[d - 1], block.at[d - 1], a_send.at[d - 1, group]).wait()


def shards(n_pair, n_aux, *args):
    la, ra, aa = args[:3]
    ina = args[6]
    le, re, ae = args[9:12]
    pairs, rows, full = aa.shape
    pairs_e, rows_e, full_e = ae.shape
    pad_e = -(-rows_e // 8) * 8
    hbm = pl.BlockSpec(memory_space=pl.ANY)
    vmem = pl.BlockSpec(memory_space=pltpu.VMEM)
    dma = pltpu.SemaphoreType.DMA
    args = list(args)
    for i in (7, 8):
        args[i] = args[i].T
    args[11] = ae.transpose(1, 0, 2)

    def like(space, *which):
        return [space(args[i].shape, args[i].dtype) for i in which]

    new_a, new_e = pl.pallas_call(
        functools.partial(kernel, n_pair, n_aux),
        out_shape=(
            pltpu.VMEM(aa.shape, F32),
            pltpu.VMEM(args[11].shape, F32),
        ),
        in_specs=[hbm] * len(args),
        out_specs=(vmem, vmem),
        scratch_shapes=like(pltpu.VMEM, 0, 1, 9, 10, 6, 2, 11, 5, 14, 15)
        + like(pltpu.SMEM, 3, 4, 7, 8, 12, 13, 16, 17)
        + [
            pltpu.VMEM((pairs, rows, full), BF),
            pltpu.VMEM((n_aux, pairs, rows, full), BF),
            pltpu.VMEM((n_pair * pairs, rows, full), BF),
            pltpu.VMEM((pairs_e, pad_e, LANES), F32),
            pltpu.VMEM((n_pair * pairs_e, pad_e, LANES), F32),
            pltpu.VMEM((pairs, n_aux, rows, full), F32),
            pltpu.VMEM((n_aux, pairs, rows, full), BF),
            pltpu.VMEM((n_aux - 1, pairs, rows, full), BF),
            pltpu.VMEM((pairs_e, full_e, full_e), F32),
            pltpu.VMEM((n_aux, pairs_e, pad_e, LANES), F32),
            pltpu.VMEM((n_aux - 1, pairs_e, pad_e, LANES), F32),
            pltpu.VMEM((pairs, rows, full), F32),
            pltpu.VMEM((pairs_e, rows_e, full_e), F32),
            pltpu.VMEM((pairs, ina.shape[1] * rows, full), BF),
            pltpu.VMEM((pairs, ina.shape[1] * rows, full), BF),
            dma((pairs, 2)),
            dma((pairs_e, 2)),
            dma,
            dma((13,)),
            dma((n_aux - 1,)),
            dma((n_aux - 1,)),
            dma((n_pair - 1,)),
            dma((n_pair - 1,)),
            dma((n_pair - 1,)),
            dma((n_pair - 1,)),
            dma((n_aux - 1, 2)),
            dma((n_aux - 1, 2)),
            dma((n_aux - 1,)),
            dma((n_aux - 1,)),
        ],
        compiler_params=pltpu.CompilerParams(
            collective_id=0, has_side_effects=True, vmem_limit_bytes=60 * 1024 * 1024
        ),
        name="update",
    )(*args)
    return new_a, new_e.transpose(1, 0, 2)


def solution(mesh):
    n_pair, n_aux = mesh.shape["pair"], mesh.shape["aux"]
    level = (
        P("pair", None, "aux"),
        P("pair", None, "aux"),
        P("pair", "aux", None),
        P("pair"),
        P("pair"),
        P("pair", None),
        P("pair", None, None, None),
        P("pair", None),
        P("pair", None),
    )
    return jax.shard_map(
        functools.partial(shards, n_pair, n_aux),
        mesh=mesh,
        in_specs=level + level,
        out_specs=(P("pair", "aux", None), P("pair", "aux", None)),
        check_vma=False,
    )
```

```python
import functools

import jax
import jax.numpy as jnp
from jax import lax
from jax.experimental import pallas as pl
from jax.experimental.pallas import tpu as pltpu
from jax.sharding import PartitionSpec as P

BF = jnp.bfloat16
F32 = jnp.float32
LANES = 128
AHEAD = 3
FIRST = 1
WARM = 5
LATE = 2
EDT = jnp.bfloat16


def dot_nt(x, y):
    return lax.dot_general(x, y, (((1,), (1,)), ((), ())), preferred_element_type=F32)


def split(x):
    hi = x.astype(BF)
    return hi, (x - hi.astype(F32)).astype(BF)


def iota2(shape, dim):
    return lax.broadcasted_iota(jnp.int32, shape, dim)


def half_couple(over, near, fock, place, rows, step):
    width = over[0].shape[1]
    pick = (iota2((step, width), 1) == place * rows + iota2((step, width), 0)) & (
        iota2((step, width), 0) < rows
    )
    pick = jnp.where(pick, F32(1.0), F32(0.0))
    lefts, rights = [], []
    for k in range(len(over)):
        both = dot_nt(jnp.concatenate([pick, near[k]], axis=0).astype(BF), over[k])
        lefts.append(both[:step])
        rights.append(both[step:] * fock[k])
    return jnp.concatenate(lefts, axis=0).astype(BF), jnp.concatenate(rights, axis=0).astype(BF)


def dot_tn(x, y):
    return lax.dot_general(x, y, (((0,), (0,)), ((), ())), preferred_element_type=F32)


def far_first(n):
    return sorted(range(1, n), key=lambda d: -min(d, n - d))


def kernel(
    n_pair, n_aux,
    la, ra, aa, rka_h, gpa_h, ena_h, ina, fka_h, nba_h,
    le, re, ae_h, rke_h, gpe_h, ene_h, ine_h, fke_h, nbe_h,
    oa, oe,
    buf, ebuf, inbuf, aabuf, ae, ena, ene, ine,
    rka, gpa, fka, nba, rke, gpe, fke, nbe,
    mine, own, around, mine_e, around_e,
    terms, out_a, in_a, terms_e, out_e, in_e, den, den_e, lefts, rights,
    load_sem, env_sem, pool, send_sem, recv_sem,
):
    pairs, rows, full = mine.shape
    rows_e, pairs_e, full_e = ae.shape
    pad_e = mine_e.shape[1]
    count = nba.shape[0]
    warm = min(WARM, pairs - 1)
    first = min(FIRST, warm)
    late = pairs - LATE
    ring = load_sem.shape[0]
    me = lax.axis_index("aux")
    my_pair = lax.axis_index("pair")
    order = far_first(n_aux)
    mesh_id = pl.DeviceIdType.MESH

    def landed(block, sem):
        pltpu.make_async_copy(block, block, sem).wait()

    def start_load(p):
        def go():
            sem = load_sem.at[p % ring if isinstance(p, int) else lax.rem(p, ring)]
            pltpu.make_async_copy(la.at[p], buf.at[p, 0], sem).start()
            pltpu.make_async_copy(ra.at[p], buf.at[p, 1], sem).start()

        if not isinstance(p, int):
            pl.when(p < pairs)(go)
        elif p < pairs:
            go()

    small = [(aa, aabuf), (rka_h, rka), (ae_h, ae), (rke_h, rke)]
    rest = [
        (gpa_h, gpa), (ena_h, ena), (fka_h, fka), (nba_h, nba), (gpe_h, gpe), (ene_h, ene),
        (ine_h, ine), (fke_h, fke), (nbe_h, nbe), (ina, inbuf),
    ]
    small = [pltpu.make_async_copy(x, y, pool.at[i]) for i, (x, y) in enumerate(small)]
    rest = [pltpu.make_async_copy(x, y, pool.at[i]) for i, (x, y) in enumerate(rest)]
    for copy in small:
        copy.start()
    barrier = pltpu.get_barrier_semaphore()
    for d in order:
        pl.semaphore_signal(barrier, inc=1, device_id={"aux": lax.rem(me + d, n_aux)}, device_id_type=mesh_id)
    for d in range(1, n_pair):
        pl.semaphore_signal(barrier, inc=1, device_id={"pair": lax.rem(my_pair + d, n_pair)}, device_id_type=mesh_id)
    for q in range(pairs_e):
        pltpu.make_async_copy(le.at[q], ebuf.at[q, 0], env_sem.at[q]).start()
        pltpu.make_async_copy(re.at[q], ebuf.at[q, 1], env_sem.at[q]).start()
    for p in range(AHEAD - 2):
        start_load(p)
    for copy in small:
        copy.wait()
    for copy in rest:
        copy.start()

    def inside(rank, start, shape):
        return (start + iota2(shape, 0) < rank) & (iota2(shape, 1) < rank)

    for p in range(pairs):
        keep = inside(rka[p], me * rows, (rows, full))
        block = jnp.where(keep, aabuf[p].astype(F32), F32(0.0)).astype(BF)
        mine[p] = block
        own[me, p] = block
        around[my_pair * pairs + p] = block
    mine_e[...] = jnp.zeros(mine_e.shape, F32)
    amps_e = ae[...].astype(F32)
    for p in range(pairs_e):
        keep = inside(rke[p], me * rows_e, (rows_e, full_e))
        mine_e[p, :rows_e, :full_e] = jnp.where(keep, amps_e[:, p, :], F32(0.0))
    for p in range(pairs_e):
        around_e[my_pair * pairs_e + p] = mine_e[p]
    out_e[...] = jnp.zeros(out_e.shape, out_e.dtype)

    def remote(src, dst, send, recv, axis, peer):
        return pltpu.make_async_remote_copy(
            src_ref=src, dst_ref=dst, send_sem=send, recv_sem=recv,
            device_id={axis: peer}, device_id_type=mesh_id,
        )

    with jax.named_scope("w_barrier"):
        pl.semaphore_wait(barrier, n_aux - 1 + n_pair - 1)
    for d in order:
        remote(mine, own.at[me], send_sem.at[0], recv_sem.at[0], "aux", lax.rem(me + d, n_aux)).start()
    for d in range(1, n_pair):
        peer = lax.rem(my_pair + d, n_pair)
        remote(mine, around.at[pl.ds(my_pair * pairs, pairs)], send_sem.at[1], recv_sem.at[1], "pair", peer).start()
        remote(mine_e, around_e.at[pl.ds(my_pair * pairs_e, pairs_e)], send_sem.at[2], recv_sem.at[2], "pair", peer).start()

    def denominators(energy, gap, start, height, wide):
        line = energy + jnp.zeros((height, wide), F32)
        diag = iota2((height, wide), 1) == start + iota2((height, wide), 0)
        mine_rows = jnp.sum(jnp.where(diag, line, F32(0.0)), axis=1, keepdims=True)
        return line + mine_rows + gap

    def send_pair(p, group):
        for d in order:
            peer = lax.rem(me + d, n_aux)
            remote(out_a.at[peer, p], in_a.at[d - 1, p], pool.at[0], recv_sem.at[3 + group], "aux", peer).start()

    def ladder(p):
        with jax.named_scope("w_load"):
            landed(buf.at[p], load_sem.at[p % ring if isinstance(p, int) else lax.rem(p, ring)])
        terms[p] = dot_nt(buf[p, 0], buf[p, 1]).reshape(n_aux, rows, full)

    def prepare(p):
        left, right = half_couple(
            [inbuf[p, k] for k in range(count)],
            [around[nba[k, p]].astype(F32) for k in range(count)],
            [fka[k, p] for k in range(count)],
            me, rows, rows,
        )
        lefts[p] = left
        rights[p] = right

    def prepare_e(q):
        left, right = half_couple(
            [ine[q, k] for k in range(count)],
            [around_e[nbe[q, k]][:, :full_e] for k in range(count)],
            [fke[q, k] for k in range(count)],
            me, rows_e, pad_e,
        )
        total = terms_e[q] + dot_tn(left, right)
        for j in range(n_aux):
            out_e[j, q, :rows_e, :full_e] = total[j * rows_e : (j + 1) * rows_e, :].astype(out_e.dtype)

    def finish(p):
        base = terms[p].reshape(full, full)
        amps = own[:, p].astype(F32).reshape(full, full).astype(BF)
        half = base + dot_nt(base.astype(BF), amps)
        total = base + dot_tn(
            jnp.concatenate([amps, lefts[p]], axis=0),
            jnp.concatenate([half.astype(BF), rights[p]], axis=0),
        )
        terms[p] = total.reshape(n_aux, rows, full)
        for j in range(n_aux):
            out_a[j, p] = total[j * rows : (j + 1) * rows].astype(BF)

    def env_step(q, carry):
        landed(ebuf.at[q], env_sem.at[q])
        terms_e[q] = dot_nt(ebuf[q, 0], ebuf[q, 1])
        return carry

    half_e = pairs_e // 2
    lax.fori_loop(0, half_e, env_step, 0)
    start_load(AHEAD - 2)
    lax.fori_loop(half_e, pairs_e, env_step, 0)
    start_load(AHEAD - 1)

    def warm_step(p, carry):
        start_load(p + AHEAD)
        ladder(p)
        return carry

    lax.fori_loop(0, first, warm_step, 0)

    with jax.named_scope("w_rest"):
        for copy in rest:
            copy.wait()
    with jax.named_scope("w_pair"):
        landed(around.at[pl.ds(0, (n_pair - 1) * pairs)], recv_sem.at[1])
        landed(around_e.at[pl.ds(0, (n_pair - 1) * pairs_e)], recv_sem.at[2])

    beside = warm - first
    share, share_e = -(-pairs // beside), -(-pairs_e // beside)

    def prepare_step(i, carry):
        start_load(first + i + AHEAD)
        ladder(first + i)
        for n in range(share):
            prepare(lax.min(share * i + n, pairs - 1))
        for n in range(share_e):
            prepare_e(lax.min(share_e * i + n, pairs_e - 1))
        return carry

    lax.fori_loop(0, beside, prepare_step, 0)
    for d in order:
        peer = lax.rem(me + d, n_aux)
        remote(out_e.at[peer], in_e.at[d - 1], pool.at[1], recv_sem.at[5], "aux", peer).start()

    for p in range(pairs):
        den[p] = denominators(ena[pl.ds(p, 1), :], gpa[p], me * rows, rows, full)
    for p in range(pairs_e):
        den_e[p] = denominators(ene[pl.ds(p, 1), :], gpe[p], me * rows_e, rows_e, full_e)
    with jax.named_scope("w_own"):
        landed(own.at[pl.ds(0, n_aux - 1)], recv_sem.at[0])

    twos = min(pairs - 1 - warm, max(0, warm - 1))

    def catch_step(i, carry):
        p = warm + i
        start_load(p + AHEAD)

        @pl.when(i > 0)
        def _():
            send_pair(2 * i - 2, 0)
            send_pair(2 * i - 1, 0)

        ladder(p)
        finish(2 * i)
        finish(2 * i + 1)
        return carry

    lax.fori_loop(0, twos, catch_step, 0)
    done = 2 * twos
    sent = max(0, done - 2)
    for p in range(warm + twos, pairs):
        start_load(p + AHEAD)
        for q in range(sent, done):
            send_pair(q, int(q >= late))
        sent = done
        ladder(p)
        if done < p:
            finish(done)
            done += 1
    while done < pairs:
        for q in range(sent, done):
            send_pair(q, int(q >= late))
        sent = done
        finish(done)
        done += 1
    for p in range(sent, pairs):
        send_pair(p, int(p >= late))

    def combine(p):
        total = terms[p, me]
        for d in range(1, n_aux):
            total = total + in_a[d - 1, p].astype(F32)
        keep = inside(rka[p], me * rows, (rows, full))
        oa[p] = jnp.where(keep, mine[p].astype(F32) - total / den[p], F32(0.0))

    with jax.named_scope("w_e"):
        landed(in_e, recv_sem.at[5])
    for p in range(pairs_e):
        total = out_e[me, p].astype(F32)
        for d in range(1, n_aux):
            total = total + in_e[d - 1, p].astype(F32)
        keep = inside(rke[p], me * rows_e, (rows_e, full_e))
        oe[:, p, :] = jnp.where(
            keep, mine_e[p, :rows_e, :full_e] - total[:rows_e, :full_e] / den_e[p], F32(0.0)
        )
    with jax.named_scope("w_a0"):
        landed(in_a.at[:, pl.ds(0, late)], recv_sem.at[3])
    for p in range(late):
        combine(p)
    with jax.named_scope("w_send"):
        landed(own.at[pl.ds(0, n_aux - 1)], send_sem.at[0])
        landed(around.at[pl.ds(0, (n_pair - 1) * pairs)], send_sem.at[1])
        landed(around_e.at[pl.ds(0, (n_pair - 1) * pairs_e)], send_sem.at[2])
        landed(in_e, pool.at[1])
        landed(in_a, pool.at[0])
    with jax.named_scope("w_a1"):
        landed(in_a.at[:, pl.ds(late, pairs - late)], recv_sem.at[4])
    for p in range(late, pairs):
        combine(p)


def store(a, e, oa, oe, sem):
    copies = [pltpu.make_async_copy(a, oa, sem.at[0]), pltpu.make_async_copy(e, oe, sem.at[1])]
    for copy in copies:
        copy.start()
    for copy in copies:
        copy.wait()


def shards(n_pair, n_aux, *args):
    la, ra, aa = args[:3]
    ina = args[6]
    le, re, ae = args[9:12]
    pairs, rows, full = aa.shape
    pairs_e, rows_e, full_e = ae.shape
    pad_e = -(-rows_e // 8) * 8
    hbm = pl.BlockSpec(memory_space=pl.ANY)
    vmem = pl.BlockSpec(memory_space=pltpu.VMEM)
    dma = pltpu.SemaphoreType.DMA
    args = list(args)
    for i in (7, 8):
        args[i] = args[i].T
    args[11] = ae.transpose(1, 0, 2)

    def like(space, *which):
        return [space(args[i].shape, args[i].dtype) for i in which]

    new_a, new_e = pl.pallas_call(
        functools.partial(kernel, n_pair, n_aux),
        out_shape=(
            pltpu.VMEM(aa.shape, F32),
            pltpu.VMEM(args[11].shape, F32),
        ),
        in_specs=[hbm] * len(args),
        out_specs=(vmem, vmem),
        scratch_shapes=[
            pltpu.VMEM((pairs, 2, *la.shape[1:]), BF),
            pltpu.VMEM((pairs_e, 2, *le.shape[1:]), BF),
        ]
        + like(pltpu.VMEM, 6, 2, 11, 5, 14, 15)
        + like(pltpu.SMEM, 3, 4, 7, 8, 12, 13, 16, 17)
        + [
            pltpu.VMEM((pairs, rows, full), BF),
            pltpu.VMEM((n_aux, pairs, rows, full), BF),
            pltpu.VMEM((n_pair * pairs, rows, full), BF),
            pltpu.VMEM((pairs_e, pad_e, LANES), F32),
            pltpu.VMEM((n_pair * pairs_e, pad_e, LANES), F32),
            pltpu.VMEM((pairs, n_aux, rows, full), F32),
            pltpu.VMEM((n_aux, pairs, rows, full), BF),
            pltpu.VMEM((n_aux - 1, pairs, rows, full), BF),
            pltpu.VMEM((pairs_e, full_e, full_e), F32),
            pltpu.VMEM((n_aux, pairs_e, pad_e, LANES), EDT),
            pltpu.VMEM((n_aux - 1, pairs_e, pad_e, LANES), EDT),
            pltpu.VMEM((pairs, rows, full), F32),
            pltpu.VMEM((pairs_e, rows_e, full_e), F32),
            pltpu.VMEM((pairs, ina.shape[1] * rows, full), BF),
            pltpu.VMEM((pairs, ina.shape[1] * rows, full), BF),
            dma((AHEAD + 1,)),
            dma((pairs_e,)),
            dma((10,)),
            dma((3,)),
            dma((6,)),
        ],
        compiler_params=pltpu.CompilerParams(
            collective_id=0, has_side_effects=True, vmem_limit_bytes=60 * 1024 * 1024
        ),
        name="update",
    )(*args)
    new_a, new_e = (pltpu.with_memory_space_constraint(x, pltpu.VMEM) for x in (new_a, new_e))
    out_a, out_e = pl.pallas_call(
        store,
        out_shape=(
            jax.ShapeDtypeStruct(new_a.shape, F32),
            jax.ShapeDtypeStruct(new_e.shape, F32),
        ),
        in_specs=[vmem, vmem],
        out_specs=(hbm, hbm),
        scratch_shapes=[dma((2,))],
        name="store",
    )(new_a, new_e)
    return out_a, out_e.transpose(1, 0, 2)


def solution(mesh):
    n_pair, n_aux = mesh.shape["pair"], mesh.shape["aux"]
    level = (
        P("pair", None, "aux"),
        P("pair", None, "aux"),
        P("pair", "aux", None),
        P("pair"),
        P("pair"),
        P("pair", None),
        P("pair", None, None, None),
        P("pair", None),
        P("pair", None),
    )
    return jax.shard_map(
        functools.partial(shards, n_pair, n_aux),
        mesh=mesh,
        in_specs=level + level,
        out_specs=(P("pair", "aux", None), P("pair", "aux", None)),
        check_vma=False,
    )
```

```python
import functools

import jax
import jax.numpy as jnp
from jax import lax
from jax.experimental import pallas as pl
from jax.experimental.pallas import tpu as pltpu
from jax.sharding import PartitionSpec as P

BF = jnp.bfloat16
F32 = jnp.float32
LANES = 128
AHEAD = 3
FIRST = 1
WARM = 5
LATE = 2
EDT = jnp.bfloat16


def dot_nt(x, y):
    return lax.dot_general(x, y, (((1,), (1,)), ((), ())), preferred_element_type=F32)


def split(x):
    hi = x.astype(BF)
    return hi, (x - hi.astype(F32)).astype(BF)


def iota2(shape, dim):
    return lax.broadcasted_iota(jnp.int32, shape, dim)


def half_couple(over, near, fock, place, rows, step):
    width = over[0].shape[1]
    pick = (iota2((step, width), 1) == place * rows + iota2((step, width), 0)) & (
        iota2((step, width), 0) < rows
    )
    pick = jnp.where(pick, F32(1.0), F32(0.0))
    lefts, rights = [], []
    for k in range(len(over)):
        both = dot_nt(jnp.concatenate([pick, near[k]], axis=0).astype(BF), over[k])
        lefts.append(both[:step])
        rights.append(both[step:] * fock[k])
    return jnp.concatenate(lefts, axis=0).astype(BF), jnp.concatenate(rights, axis=0).astype(BF)


def dot_tn(x, y):
    return lax.dot_general(x, y, (((0,), (0,)), ((), ())), preferred_element_type=F32)


def kernel(
    n_pair, n_aux,
    la, ra, aa, rka_h, gpa_h, ena_h, ina, fka_h, nba_h,
    le, re, ae_h, rke_h, gpe_h, ene_h, ine_h, fke_h, nbe_h,
    oa, oe,
    buf, ebuf, inbuf, aabuf, ae, ena, ene, ine,
    rka, gpa, fka, nba, rke, gpe, fke, nbe,
    mine, own, around, mine_e, around_e,
    terms, out_a, in_a, terms_e, out_e, in_e, den, den_e, lefts, rights,
    load_sem, env_sem, pool, send_sem, recv_sem,
):
    pairs, rows, full = mine.shape
    rows_e, pairs_e, full_e = ae.shape
    pad_e = mine_e.shape[1]
    count = nba.shape[0]
    warm = min(WARM, pairs - 1)
    first = min(FIRST, warm)
    late = pairs - LATE
    ring = load_sem.shape[0]
    me = lax.axis_index("aux")
    my_pair = lax.axis_index("pair")
    order = range(1, n_aux)
    mesh_id = pl.DeviceIdType.MESH

    def landed(block, sem):
        pltpu.make_async_copy(block, block, sem).wait()

    def start_load(p):
        def go():
            sem = load_sem.at[p % ring if isinstance(p, int) else lax.rem(p, ring)]
            pltpu.make_async_copy(la.at[p], buf.at[p, 0], sem).start()
            pltpu.make_async_copy(ra.at[p], buf.at[p, 1], sem).start()

        if not isinstance(p, int):
            pl.when(p < pairs)(go)
        elif p < pairs:
            go()

    small = [(aa, aabuf), (rka_h, rka), (ae_h, ae), (rke_h, rke)]
    rest = [
        (gpa_h, gpa), (ena_h, ena), (fka_h, fka), (nba_h, nba), (gpe_h, gpe), (ene_h, ene),
        (ine_h, ine), (fke_h, fke), (nbe_h, nbe), (ina, inbuf),
    ]
    small = [pltpu.make_async_copy(x, y, pool.at[i]) for i, (x, y) in enumerate(small)]
    rest = [pltpu.make_async_copy(x, y, pool.at[i]) for i, (x, y) in enumerate(rest)]
    for copy in small:
        copy.start()
    barrier = pltpu.get_barrier_semaphore()
    for d in order:
        pl.semaphore_signal(barrier, inc=1, device_id={"aux": lax.rem(me + d, n_aux)}, device_id_type=mesh_id)
    for d in range(1, n_pair):
        pl.semaphore_signal(barrier, inc=1, device_id={"pair": lax.rem(my_pair + d, n_pair)}, device_id_type=mesh_id)
    for q in range(pairs_e):
        pltpu.make_async_copy(le.at[q], ebuf.at[q, 0], env_sem.at[q]).start()
        pltpu.make_async_copy(re.at[q], ebuf.at[q, 1], env_sem.at[q]).start()
    for p in range(AHEAD - 2):
        start_load(p)
    for copy in small:
        copy.wait()
    for copy in rest:
        copy.start()

    def inside(rank, start, shape):
        return (start + iota2(shape, 0) < rank) & (iota2(shape, 1) < rank)

    for p in range(pairs):
        keep = inside(rka[p], me * rows, (rows, full))
        block = jnp.where(keep, aabuf[p].astype(F32), F32(0.0)).astype(BF)
        mine[p] = block
        own[me, p] = block
        around[my_pair * pairs + p] = block
    mine_e[...] = jnp.zeros(mine_e.shape, BF)
    amps_e = ae[...].astype(F32)
    for p in range(pairs_e):
        keep = inside(rke[p], me * rows_e, (rows_e, full_e))
        mine_e[p, :rows_e, :full_e] = jnp.where(keep, amps_e[:, p, :], F32(0.0)).astype(BF)
    for p in range(pairs_e):
        around_e[my_pair * pairs_e + p] = mine_e[p]
    out_e[...] = jnp.zeros(out_e.shape, out_e.dtype)

    def remote(src, dst, send, recv, axis, peer):
        return pltpu.make_async_remote_copy(
            src_ref=src, dst_ref=dst, send_sem=send, recv_sem=recv,
            device_id={axis: peer}, device_id_type=mesh_id,
        )

    with jax.named_scope("w_barrier"):
        pl.semaphore_wait(barrier, n_aux - 1 + n_pair - 1)
    for d in range(1, n_pair):
        peer = lax.rem(my_pair + d, n_pair)
        remote(mine, around.at[pl.ds(my_pair * pairs, pairs)], send_sem.at[1], recv_sem.at[1], "pair", peer).start()
        remote(mine_e, around_e.at[pl.ds(my_pair * pairs_e, pairs_e)], send_sem.at[2], recv_sem.at[2], "pair", peer).start()
    for d in order:
        remote(mine, own.at[me], send_sem.at[0], recv_sem.at[0], "aux", lax.rem(me + d, n_aux)).start()

    def denominators(energy, gap, start, height, wide):
        line = energy + jnp.zeros((height, wide), F32)
        diag = iota2((height, wide), 1) == start + iota2((height, wide), 0)
        mine_rows = jnp.sum(jnp.where(diag, line, F32(0.0)), axis=1, keepdims=True)
        return line + mine_rows + gap

    def send_pair(p, group, some=1):
        for d in order:
            peer = lax.rem(me + d, n_aux)
            remote(
                out_a.at[peer, pl.ds(p, some)], in_a.at[d - 1, pl.ds(p, some)],
                pool.at[0], recv_sem.at[3 + group], "aux", peer,
            ).start()

    def ladder(p):
        with jax.named_scope("w_load"):
            landed(buf.at[p], load_sem.at[p % ring if isinstance(p, int) else lax.rem(p, ring)])
        terms[p] = dot_nt(buf[p, 0], buf[p, 1]).reshape(n_aux, rows, full)

    def prepare(p):
        left, right = half_couple(
            [inbuf[p, k] for k in range(count)],
            [around[nba[k, p]].astype(F32) for k in range(count)],
            [fka[k, p] for k in range(count)],
            me, rows, rows,
        )
        lefts[p] = left
        rights[p] = right

    def prepare_e(q):
        left, right = half_couple(
            [ine[q, k] for k in range(count)],
            [around_e[nbe[q, k]].astype(F32)[:, :full_e] for k in range(count)],
            [fke[q, k] for k in range(count)],
            me, rows_e, pad_e,
        )
        total = terms_e[q] + dot_tn(left, right)
        for j in range(n_aux):
            out_e[j, q, :rows_e, :full_e] = total[j * rows_e : (j + 1) * rows_e, :].astype(out_e.dtype)

    def finish(p):
        base = terms[p].reshape(full, full)
        amps = own[:, p].astype(F32).reshape(full, full).astype(BF)
        half = base + dot_nt(base.astype(BF), amps)
        total = base + dot_tn(
            jnp.concatenate([amps, lefts[p]], axis=0),
            jnp.concatenate([half.astype(BF), rights[p]], axis=0),
        )
        terms[p] = total.reshape(n_aux, rows, full)
        for j in range(n_aux):
            out_a[j, p] = total[j * rows : (j + 1) * rows].astype(BF)

    def env_step(q, carry):
        landed(ebuf.at[q], env_sem.at[q])
        terms_e[q] = dot_nt(ebuf[q, 0], ebuf[q, 1])
        return carry

    half_e = pairs_e // 2
    lax.fori_loop(0, half_e, env_step, 0)
    start_load(AHEAD - 2)
    lax.fori_loop(half_e, pairs_e, env_step, 0)
    start_load(AHEAD - 1)

    def warm_step(p, carry):
        start_load(p + AHEAD)
        ladder(p)
        return carry

    lax.fori_loop(0, first, warm_step, 0)

    with jax.named_scope("w_rest"):
        for copy in rest:
            copy.wait()
    with jax.named_scope("w_pair"):
        landed(around.at[pl.ds(0, (n_pair - 1) * pairs)], recv_sem.at[1])
        landed(around_e.at[pl.ds(0, (n_pair - 1) * pairs_e)], recv_sem.at[2])

    beside = warm - first
    share, share_e = -(-pairs // beside), -(-pairs_e // beside)

    def prepare_step(i, carry):
        start_load(first + i + AHEAD)
        ladder(first + i)
        for n in range(share):
            prepare(lax.min(share * i + n, pairs - 1))
        for n in range(share_e):
            prepare_e(lax.min(share_e * i + n, pairs_e - 1))
        return carry

    lax.fori_loop(0, beside, prepare_step, 0)
    for d in order:
        peer = lax.rem(me + d, n_aux)
        remote(out_e.at[peer], in_e.at[d - 1], pool.at[1], recv_sem.at[5], "aux", peer).start()

    for p in range(pairs):
        den[p] = denominators(ena[pl.ds(p, 1), :], gpa[p], me * rows, rows, full)
    for p in range(pairs_e):
        den_e[p] = denominators(ene[pl.ds(p, 1), :], gpe[p], me * rows_e, rows_e, full_e)
    with jax.named_scope("w_own"):
        landed(own.at[pl.ds(0, n_aux - 1)], recv_sem.at[0])

    twos = min(pairs - 1 - warm, max(0, warm - 1))

    def catch_step(i, carry):
        p = warm + i
        start_load(p + AHEAD)

        @pl.when(i > 0)
        def _():
            send_pair(2 * i - 2, 0, 2)

        ladder(p)
        finish(2 * i)
        finish(2 * i + 1)
        return carry

    lax.fori_loop(0, twos, catch_step, 0)
    done = 2 * twos
    sent = max(0, done - 2)
    for p in range(warm + twos, pairs):
        start_load(p + AHEAD)
        if sent < done:
            send_pair(sent, int(sent >= late), done - sent)
        sent = done
        ladder(p)
        if done < p:
            finish(done)
            done += 1
    while done < pairs:
        for q in range(sent, done):
            send_pair(q, int(q >= late))
        sent = done
        finish(done)
        done += 1
    for p in range(sent, pairs):
        send_pair(p, int(p >= late))

    def combine(p):
        total = terms[p, me]
        for d in range(1, n_aux):
            total = total + in_a[d - 1, p].astype(F32)
        keep = inside(rka[p], me * rows, (rows, full))
        oa[p] = jnp.where(keep, mine[p].astype(F32) - total / den[p], F32(0.0))

    with jax.named_scope("w_e"):
        landed(in_e, recv_sem.at[5])
    for p in range(pairs_e):
        total = out_e[me, p].astype(F32)
        for d in range(1, n_aux):
            total = total + in_e[d - 1, p].astype(F32)
        keep = inside(rke[p], me * rows_e, (rows_e, full_e))
        oe[:, p, :] = jnp.where(
            keep, mine_e[p].astype(F32)[:rows_e, :full_e] - total[:rows_e, :full_e] / den_e[p], F32(0.0)
        )
    with jax.named_scope("w_a0"):
        landed(in_a.at[:, pl.ds(0, late)], recv_sem.at[3])
    for p in range(late):
        combine(p)
    with jax.named_scope("w_send"):
        landed(own.at[pl.ds(0, n_aux - 1)], send_sem.at[0])
        landed(around.at[pl.ds(0, (n_pair - 1) * pairs)], send_sem.at[1])
        landed(around_e.at[pl.ds(0, (n_pair - 1) * pairs_e)], send_sem.at[2])
        landed(in_e, pool.at[1])
        landed(in_a, pool.at[0])
    with jax.named_scope("w_a1"):
        landed(in_a.at[:, pl.ds(late, pairs - late)], recv_sem.at[4])
    for p in range(late, pairs):
        combine(p)


def store(a, e, oa, oe, sem):
    copies = [pltpu.make_async_copy(a, oa, sem.at[0]), pltpu.make_async_copy(e, oe, sem.at[1])]
    for copy in copies:
        copy.start()
    for copy in copies:
        copy.wait()


def shards(n_pair, n_aux, *args):
    la, ra, aa = args[:3]
    ina = args[6]
    le, re, ae = args[9:12]
    pairs, rows, full = aa.shape
    pairs_e, rows_e, full_e = ae.shape
    pad_e = -(-rows_e // 8) * 8
    hbm = pl.BlockSpec(memory_space=pl.ANY)
    vmem = pl.BlockSpec(memory_space=pltpu.VMEM)
    dma = pltpu.SemaphoreType.DMA
    args = list(args)
    for i in (7, 8):
        args[i] = args[i].T
    args[11] = ae.transpose(1, 0, 2)

    def like(space, *which):
        return [space(args[i].shape, args[i].dtype) for i in which]

    new_a, new_e = pl.pallas_call(
        functools.partial(kernel, n_pair, n_aux),
        out_shape=(
            pltpu.VMEM(aa.shape, F32),
            pltpu.VMEM(args[11].shape, F32),
        ),
        in_specs=[hbm] * len(args),
        out_specs=(vmem, vmem),
        scratch_shapes=[
            pltpu.VMEM((pairs, 2, *la.shape[1:]), BF),
            pltpu.VMEM((pairs_e, 2, *le.shape[1:]), BF),
        ]
        + like(pltpu.VMEM, 6, 2, 11, 5, 14, 15)
        + like(pltpu.SMEM, 3, 4, 7, 8, 12, 13, 16, 17)
        + [
            pltpu.VMEM((pairs, rows, full), BF),
            pltpu.VMEM((n_aux, pairs, rows, full), BF),
            pltpu.VMEM((n_pair * pairs, rows, full), BF),
            pltpu.VMEM((pairs_e, pad_e, LANES), BF),
            pltpu.VMEM((n_pair * pairs_e, pad_e, LANES), BF),
            pltpu.VMEM((pairs, n_aux, rows, full), F32),
            pltpu.VMEM((n_aux, pairs, rows, full), BF),
            pltpu.VMEM((n_aux - 1, pairs, rows, full), BF),
            pltpu.VMEM((pairs_e, full_e, full_e), F32),
            pltpu.VMEM((n_aux, pairs_e, pad_e, LANES), EDT),
            pltpu.VMEM((n_aux - 1, pairs_e, pad_e, LANES), EDT),
            pltpu.VMEM((pairs, rows, full), F32),
            pltpu.VMEM((pairs_e, rows_e, full_e), F32),
            pltpu.VMEM((pairs, ina.shape[1] * rows, full), BF),
            pltpu.VMEM((pairs, ina.shape[1] * rows, full), BF),
            dma((AHEAD + 1,)),
            dma((pairs_e,)),
            dma((10,)),
            dma((3,)),
            dma((6,)),
        ],
        compiler_params=pltpu.CompilerParams(
            collective_id=0, has_side_effects=True, vmem_limit_bytes=60 * 1024 * 1024
        ),
        name="update",
    )(*args)
    new_a, new_e = (pltpu.with_memory_space_constraint(x, pltpu.VMEM) for x in (new_a, new_e))
    out_a, out_e = pl.pallas_call(
        store,
        out_shape=(
            jax.ShapeDtypeStruct(new_a.shape, F32),
            jax.ShapeDtypeStruct(new_e.shape, F32),
        ),
        in_specs=[vmem, vmem],
        out_specs=(hbm, hbm),
        scratch_shapes=[dma((2,))],
        name="store",
    )(new_a, new_e)
    return out_a, out_e.transpose(1, 0, 2)


def solution(mesh):
    n_pair, n_aux = mesh.shape["pair"], mesh.shape["aux"]
    level = (
        P("pair", None, "aux"),
        P("pair", None, "aux"),
        P("pair", "aux", None),
        P("pair"),
        P("pair"),
        P("pair", None),
        P("pair", None, None, None),
        P("pair", None),
        P("pair", None),
    )
    return jax.shard_map(
        functools.partial(shards, n_pair, n_aux),
        mesh=mesh,
        in_specs=level + level,
        out_specs=(P("pair", "aux", None), P("pair", "aux", None)),
        check_vma=False,
    )
```
